128 devices in a mesh: row: 8 (over z, y_lo), col: 16 (over x, y_hi, core).
Axes of the slice: x: 4, y: 4 (y_hi: 2, y_lo: 2; y = y_hi * 2 + y_lo), z: 4, core: 2. Of those that a mesh axis runs over, the one named last changes fastest.
Arguments:
- right_side: float32 [512, 512, 512], P(('row', 'col')), may hold values from -51 to 51
- coupling: float32 [512, 512, 512], P(('row', 'col')), may hold values from 0.01 to 0.3
Outputs:
- solution: float32 [512, 512, 512], P(('row', 'col'))
- residual: float32 [512, 512, 512], P(('row', 'col'))
- residual_norm: float32 [1], replicated
The draws below stay inside these ranges and needn't reach their ends.
All inputs are finite; a program needn't handle non-finite values.
Results may differ from the reference program's by a relative error of at most 0.0003.
Values sent between devices are 32-bit elements; how exact they have to be, the bound alone decides.
A program may use at most 128 MiB of HBM per device.

```python
import math
import jax
import jax.numpy as jnp

NX = 512
NY = 512
NZ = 512


def draw_right_side(key, part):
    base_key = jax.random.fold_in(key, 101)
    first_key, second_key = jax.random.split(base_key)
    plane = jnp.arange(NZ).astype(jnp.float32) / NZ
    zscale = jnp.exp((plane - 0.5) * math.log(10.0))
    xscale = jnp.exp(jax.random.uniform(second_key, (NX,), jnp.float32, -0.5 * math.log(10.0), 0.5 * math.log(10.0)))
    base = jnp.clip(jax.random.normal(first_key, (NZ, NY, NX), jnp.float32), -5.0, 5.0)
    return (base * zscale[:, None, None] * xscale[None, None, :]).astype(jnp.float32)


def levels(rng, extent, shards, low, largest):
    loudness, own = 1.0, jax.random.fold_in(rng, 6)
    for position, blocks in shards:
        steps = jnp.exp(jax.random.uniform(jax.random.fold_in(own, position), (blocks,), jnp.float32, low / len(shards), largest / len(shards)))
        loudness = loudness * jnp.repeat(steps, extent[position] // blocks).reshape([-1 if axis == position else 1 for axis in range(len(extent))])
    return loudness


def setup_inputs(seed: int = 0) -> dict:
    key_of = jax.random.split(jax.random.key(seed), 3)
    return {
        "right_side": draw_right_side(jax.random.fold_in(key_of[2], 71), 0),
        "coupling": jnp.clip(jnp.exp(math.log(0.3) - 3.4011974 * jax.random.uniform(key_of[1], (NZ, NY, NX), jnp.float32) ** levels(key_of[1], (NZ, NY, NX), ((0, 128),), -0.2, 0.2)), 0.01, 0.3),
    }


def hartley(field, axis):
    spectral = jnp.fft.fft(field, axis=axis)
    return jnp.real(spectral) - jnp.imag(spectral)

def wave_square(count):
    index = jnp.arange(count).astype(jnp.int32)
    signed = jnp.where(2 * index < count, index, index - count).astype(jnp.float32)
    return jnp.square(signed * (2.0 * math.pi / count))

def reference(right_side, coupling):
    spectrum = hartley(hartley(hartley(right_side, 2), 1), 0)
    eigen = wave_square(NZ)[:, None, None] + wave_square(NY)[None, :, None] + wave_square(NX)[None, None, :]
    volume = float(NX * NY * NZ)
    positive = eigen > 0
    scaled = jnp.where(positive, spectrum / jnp.where(positive, eigen * volume, 1.0), 0.0)
    solution = hartley(hartley(hartley(scaled, 0), 1), 2)
    lap = 6.0 * solution
    for axis in range(3):
        lap = lap - jnp.roll(solution, 1, axis) - jnp.roll(solution, -1, axis)
    residual = right_side - (coupling * solution + lap)
    residual_norm = jnp.sqrt(jnp.sum(residual * residual)).reshape(1)
    return (solution, residual, residual_norm)
```

```python
import math

import jax
import jax.numpy as jnp
from jax import lax
from jax.experimental import pallas as pl
from jax.experimental.pallas import tpu as pltpu
from jax.sharding import PartitionSpec as P

ROW_COL = ("row", "col")
MESH = pl.DeviceIdType.MESH


HIGHEST = lax.Precision.HIGHEST


def with_halo(x, sides, width):
    edges = {}
    for axis, dim in sides:
        size, length = (lax.axis_size(axis), x.shape[dim])
        up = [(i, (i + 1) % size) for i in range(size)]
        last = lax.slice_in_dim(x, length - width, length, axis=dim)
        initial = lax.slice_in_dim(x, 0, width, axis=dim)
        edges[dim] = (
            lax.ppermute(last, axis, up),
            lax.ppermute(initial, axis, [(b, a) for a, b in up]),
        )
    done = []
    for _, dim in sides:
        low, high = edges[dim]
        around = [(width, width) if d in done else (0, 0) for d in range(x.ndim)]
        x = jnp.concatenate([jnp.pad(low, around), x, jnp.pad(high, around)], axis=dim)
        done.append(dim)
    return x


def place():
    row, col = lax.axis_index("row"), lax.axis_index("col")
    return col // 4, (col // 2) % 2 * 2 + row % 2, row // 2, col % 2


def device(x, y, z, core):
    return z * 2 + y % 2, x * 4 + y // 2 * 2 + core


def partner(here, i):
    x, y, z, core = here
    sign = 1 - 2 * core
    dx, dy, dz = i % 4, (i // 4 + i) % 4, (i // 16 + i) % 4
    return device(
        (x + sign * dx + 4) % 4,
        (y + sign * dy + 4) % 4,
        (z + sign * dz + 4) % 4,
        (core + i // 64) % 2,
    )


def exchange_kernel(x_ref, o_ref, send_sem, recv_sem, own_sem):
    here = place()
    me = lax.axis_index("row") * 16 + lax.axis_index("col")
    barrier = pltpu.get_barrier_semaphore()

    def greet(i, carry):
        row, col = partner(here, i)
        pl.semaphore_signal(barrier, inc=1, device_id=(row, col), device_id_type=MESH)
        return carry

    lax.fori_loop(1, 128, greet, 0)
    own = pltpu.make_async_copy(x_ref.at[me], o_ref.at[me], own_sem)
    own.start()
    pl.semaphore_wait(barrier, 127)

    def send(i, carry):
        row, col = partner(here, i)
        pltpu.make_async_remote_copy(
            src_ref=x_ref.at[row * 16 + col],
            dst_ref=o_ref.at[me],
            send_sem=send_sem,
            recv_sem=recv_sem,
            device_id=(row, col),
            device_id_type=MESH,
        ).start()
        return carry

    lax.fori_loop(1, 128, send, 0)
    own.wait()
    most = pl.ds(0, 127)
    pltpu.make_async_copy(x_ref.at[most], o_ref.at[most], send_sem).wait()
    pltpu.make_async_copy(x_ref.at[most], o_ref.at[most], recv_sem).wait()


def exchange(x, ident):
    return pl.pallas_call(
        exchange_kernel,
        out_shape=jax.ShapeDtypeStruct(x.shape, x.dtype),
        in_specs=[pl.BlockSpec(memory_space=pltpu.VMEM)],
        out_specs=pl.BlockSpec(memory_space=pltpu.VMEM),
        scratch_shapes=[pltpu.SemaphoreType.DMA] * 3,
        compiler_params=pltpu.CompilerParams(collective_id=ident, has_side_effects=True),
    )(x)


def cas_table(count):
    index = jnp.arange(count, dtype=jnp.int32)
    product = index[:, None] * index[None, :] % count
    angle = product.astype(jnp.float32) * (2.0 * math.pi / count)
    return jnp.cos(angle) + jnp.sin(angle)


def wave_square(count):
    index = jnp.arange(count, dtype=jnp.int32)
    signed = jnp.where(2 * index < count, index, index - count).astype(jnp.float32)
    return jnp.square(signed * (2.0 * math.pi / count))


def along_last(field, table):
    return jnp.einsum("abx,xk->abk", field, table, precision=HIGHEST)


def along_middle(field, table):
    return jnp.einsum("ayb,yk->akb", field, table, precision=HIGHEST)


def along_first(field, table):
    return jnp.einsum("zab,zk->kab", field, table, precision=HIGHEST)


def shards(right_side, coupling):
    planes, rows, cols = right_side.shape
    depth = planes * lax.axis_size(ROW_COL)
    table_x = cas_table(cols)
    table_y = cas_table(rows)
    table_z = cas_table(depth)
    spectra = along_middle(along_last(right_side, table_x), table_y)
    pieces = spectra.reshape(4, 128, 4, 512).transpose(1, 0, 2, 3).reshape(128, 16, 512)
    pencil = exchange(pieces, 0).reshape(512, 4, 512)
    block = lax.axis_index(ROW_COL)
    width = pencil.shape[1]
    spectrum = along_first(pencil, table_z)
    start = block * width
    wave_rows = lax.dynamic_slice_in_dim(wave_square(rows), start, width, 0)
    eigen = (
        wave_square(depth)[:, None, None]
        + wave_rows[None, :, None]
        + wave_square(cols)[None, None, :]
    )
    volume = float(depth * rows * cols)
    positive = eigen > 0
    scaled = jnp.where(positive, spectrum / jnp.where(positive, eigen * volume, 1.0), 0.0)
    lines = along_first(scaled, table_z)
    slab = exchange(lines.reshape(128, 16, 512), 1)
    slab = slab.reshape(128, 4, 4, 512).transpose(1, 0, 2, 3).reshape(4, 512, 512)
    slab = along_middle(slab, table_y)
    solution = along_last(slab, table_x)
    padded = with_halo(solution, ((ROW_COL, 0),), 1)
    lap = 6.0 * solution - padded[2:] - padded[:-2]
    lap = lap - jnp.roll(solution, 1, 1) - jnp.roll(solution, -1, 1)
    lap = lap - jnp.roll(solution, 1, 2) - jnp.roll(solution, -1, 2)
    residual = right_side - (coupling * solution + lap)
    squares = lax.psum(jnp.sum(residual * residual), ROW_COL)
    residual_norm = jnp.sqrt(squares).reshape(1)
    return (solution, residual, residual_norm)


def solution(mesh):
    placed = P(ROW_COL, None, None)
    return jax.shard_map(
        shards,
        mesh=mesh,
        in_specs=(placed, placed),
        out_specs=(placed, placed, P()),
        check_vma=False,
    )
```

```python
import math

import jax
import jax.numpy as jnp
import numpy as np
from jax import lax
from jax.experimental import pallas as pl
from jax.experimental.pallas import tpu as pltpu
from jax.sharding import PartitionSpec as P

ROW_COL = ("row", "col")
MESH = pl.DeviceIdType.MESH
SIZE = 512
HALF = SIZE // 2
DEVICES = 128
OWN = SIZE // DEVICES
PLANES = OWN + 1
F32, BF16 = jnp.float32, jnp.bfloat16
EVEN, ODD, ODD_T = 0, 2, 4


def tables():
    n = np.arange(HALF)

    def cas(product):
        angle = 2.0 * math.pi * (product % SIZE) / SIZE
        return np.cos(angle) + np.sin(angle)

    parts = []
    even, odd = cas(n[:, None] * (2 * n)), cas(n[:, None] * (2 * n + 1))
    for table in (even, odd, odd.T):
        high = table.astype(BF16)
        parts += [high, (table - high.astype(np.float64)).astype(BF16)]
    return np.stack(parts)


def split(field):
    high = field.astype(BF16)
    return high, (field - high.astype(F32)).astype(BF16)


def times_right(field, tab, index):
    high, low = split(field)
    table_high, table_low = tab[index], tab[index + 1]
    return jnp.dot(
        jnp.concatenate([high, high, low], axis=1),
        jnp.concatenate([table_high, table_low, table_high], axis=0),
        preferred_element_type=F32,
    )


def times_left(tab, index, field):
    high, low = split(field)
    table_high, table_low = tab[index], tab[index + 1]
    return jnp.dot(
        jnp.concatenate([table_high, table_low, table_high], axis=1),
        jnp.concatenate([high, high, low], axis=0),
        preferred_element_type=F32,
    )


def wave(index):
    signed = jnp.where(2 * index < SIZE, index, index - SIZE).astype(F32)
    return jnp.square(signed * (2.0 * math.pi / SIZE))


def partner(me, i):
    core = me & 1
    sign = 1 - 2 * core
    y = (me & 2) | (me >> 4 & 1)
    x = ((me >> 2) + sign * i) & 3
    y = (y + sign * (i + (i >> 2))) & 3
    z = ((me >> 5) + sign * (i + (i >> 4))) & 3
    core = core ^ (i >> 6)
    return z * 2 + (y & 1), x * 4 + (y & 2) + core


def for_partners(me, act):
    def step(i, carry):
        row, col = partner(me, i)
        act(row, col, row * 16 + col)
        return carry

    lax.fori_loop(1, DEVICES, step, 0)


def kernel(
    rhs_hbm, coupling_hbm, tab_hbm,
    solution_ref, residual_ref, norm_ref,
    rhs, coupling, tab, send1, recv1, send2, recv2, part, field, sums,
    load_sem, plane_sem, own_sem, send_sem, recv_sem, pair_sem,
):
    row, col = lax.axis_index("row"), lax.axis_index("col")
    me = row * 16 + col
    core = me & 1
    load_tab = pltpu.make_async_copy(tab_hbm, tab, load_sem.at[0])
    load_coupling = pltpu.make_async_copy(coupling_hbm, coupling, load_sem.at[1])

    def load_plane(p):
        return pltpu.make_async_copy(rhs_hbm.at[p], rhs.at[p], plane_sem.at[p])

    load_tab.start()
    for p in range(OWN):
        load_plane(p).start()
    load_coupling.start()

    barrier = pltpu.get_barrier_semaphore()

    def greet(r, c, _):
        pl.semaphore_signal(barrier, inc=1, device_id=(r, c), device_id_type=MESH)

    for_partners(me, greet)

    def send(src, dst, stage, r, c):
        pltpu.make_async_remote_copy(
            src_ref=src,
            dst_ref=dst,
            send_sem=send_sem.at[stage],
            recv_sem=recv_sem.at[stage],
            device_id=(r, c),
            device_id_type=MESH,
        ).start()

    def wait_for(like, sem, stage):
        pltpu.make_async_copy(like, like, sem.at[stage]).wait()

    def rows(start, count):
        return pl.ds(pl.multiple_of(start, 8), count)

    row_mode = lax.broadcasted_iota(jnp.int32, (8, HALF), 0)
    lane_mode = lax.broadcasted_iota(jnp.int32, (8, HALF), 1)

    def forward(h):
        def plane(p, carry):
            if h == 0:
                load_plane(p).wait()
            low, high = rhs[p, :, :HALF], rhs[p, :, HALF:]
            if h == 0:
                both = low + high
                mean = jnp.sum(jnp.sum(both, axis=0, keepdims=True), axis=1, keepdims=True)
                mean = mean * (1.0 / SIZE**2)
                lines = times_right(both - 2.0 * mean, tab, EVEN)
            else:
                lines = times_right(low - high, tab, ODD)
            low, high = lines[:HALF], lines[HALF:]
            for side in range(2):
                if side == 0:
                    modes = times_left(tab, EVEN, low + high)
                    if h == 0:
                        constant = (row_mode == 0) & (lane_mode == 0)
                        top = modes[:8] + jnp.where(constant, mean * float(SIZE**2), 0.0)
                        modes = jnp.concatenate([top, modes[8:]], axis=0)
                else:
                    modes = times_left(tab, ODD_T, low - high)
                for g in range(32):
                    for q in range(2):
                        to = ((side * 32 + g) * 2 + q) * 8 * OWN
                        send1[h, rows(to + p * 8, 8)] = modes[
                            g * 8 : g * 8 + 8, q * 128 : q * 128 + 128
                        ]
            return carry

        lax.fori_loop(0, OWN, plane, 0)

    def send_forward(h):
        def piece(t):
            return send1.at[h, rows(t * 8 * OWN, 8 * OWN)]

        to = recv1.at[h, rows(me * 8 * OWN, 8 * OWN)]
        for_partners(me, lambda r, c, t: send(piece(t), to, h, r, c))
        pltpu.make_async_copy(piece(me), to, own_sem.at[h]).start()

    mode_z = lax.broadcasted_iota(jnp.int32, (HALF, 1), 0) * 2
    waves_z = (wave(mode_z), wave(mode_z + 1))
    lane = lax.broadcasted_iota(jnp.int32, (1, 128), 1)

    def along_z(h):
        wave_x = wave(2 * (me % 2 * 128 + lane) + h)

        def pair(i, carry):
            columns, wave_xy = [], []
            for b in range(2):
                columns.append(recv1[h, pl.ds(2 * i + b, SIZE, stride=8), :])
                order = lane * 0 + (me // 2 * 8 + 2 * i + b)
                mode_y = 2 * order - jnp.where(order < HALF, 0, SIZE - 1)
                wave_xy.append(wave(mode_y) + wave_x)
            lines = jnp.concatenate(columns, axis=1)
            wave_xy = jnp.concatenate(wave_xy, axis=1)
            total = jnp.sum(lines, axis=0, keepdims=True)
            lines = lines - total * (1.0 / SIZE)
            low, high = lines[:HALF], lines[HALF:]

            def scaled(spectrum, wave_z):
                eigen = wave_z + wave_xy
                positive = eigen > 0
                divisor = jnp.where(positive, eigen * float(SIZE**3), 1.0)
                inverse = 1.0 / divisor
                inverse = inverse * (2.0 - divisor * inverse)
                return jnp.where(positive, spectrum * inverse, 0.0)

            even = times_left(tab, EVEN, low + high)
            even = scaled(even + jnp.where(mode_z == 0, total, 0.0), waves_z[0])
            odd = scaled(times_left(tab, ODD_T, low - high), waves_z[1])
            even = times_left(tab, EVEN, even)
            odd = times_left(tab, ODD, odd)
            low, high = even + odd, even - odd
            for b in range(2):
                part_of = slice(b * 128, b * 128 + 128)
                at = 2 * i + b
                send2[h, pl.ds(at + 8, HALF, stride=8), :] = low[:, part_of]
                send2[h, pl.ds(at + 8 + 8 * HALF, HALF, stride=8), :] = high[:, part_of]
                send2[h, pl.ds(at, 1), :] = high[HALF - 1 :, part_of]
                send2[h, pl.ds(at + 8 + 8 * SIZE, 1), :] = low[:1, part_of]
            return carry

        lax.fori_loop(0, 4, pair, 0)

    def send_back(h):
        def piece(t):
            return send2.at[h, rows(t * 8 * OWN + t % 2 * 8, 8 * PLANES)]

        to = recv2.at[h, rows(me * 8 * PLANES, 8 * PLANES)]
        for_partners(me, lambda r, c, t: send(piece(t), to, 2 + h, r, c))
        pltpu.make_async_copy(piece(me), to, own_sem.at[2 + h]).start()

    def arrived(stage):
        if stage < 2:
            like, own = recv1.at[stage], 8 * OWN
        else:
            like, own = recv2.at[stage - 2], 8 * PLANES
        one = like.at[pl.ds(0, own)]
        pltpu.make_async_copy(one, one, own_sem.at[stage]).wait()
        most = like.at[pl.ds(0, (DEVICES - 1) * own)]
        pltpu.make_async_copy(most, most, recv_sem.at[stage]).wait()

    def sent(stage):
        like, own = (recv1, 8 * OWN) if stage < 2 else (recv2, 8 * PLANES)
        most = like.at[stage % 2, pl.ds(0, (DEVICES - 1) * own)]
        pltpu.make_async_copy(most, most, send_sem.at[stage]).wait()

    def inverse(h, j):
        columns = []
        for q in range(2):
            tiles = [
                recv2[h, rows((g * 2 + q) * 8 * PLANES + j * 8, 8)] for g in range(64)
            ]
            columns.append(jnp.concatenate(tiles, axis=0))
        modes = jnp.concatenate(columns, axis=1)
        even = times_left(tab, EVEN, modes[:HALF])
        odd = times_left(tab, ODD, modes[HALF:])
        lines = jnp.concatenate([even + odd, even - odd], axis=0)
        if h == 0:
            part[j] = times_right(lines, tab, EVEN)
        else:
            odd = times_right(lines, tab, ODD_T)
            even = part[j]
            field[j + core, :, :HALF] = even + odd
            field[j + core, :, HALF:] = even - odd

    load_tab.wait()
    forward(0)
    pl.semaphore_wait(barrier, DEVICES - 1)
    send_forward(0)
    forward(1)
    send_forward(1)
    arrived(0)
    along_z(0)
    arrived(1)
    send_back(0)
    along_z(1)
    send_back(1)

    arrived(2)

    def first_half(j, carry):
        inverse(0, j)
        return carry

    lax.fori_loop(0, PLANES, first_half, 0)
    arrived(3)
    swap = pltpu.make_async_remote_copy(
        src_ref=field.at[OWN - (OWN - 1) * core],
        dst_ref=field.at[(OWN + 1) * core],
        send_sem=pair_sem.at[0],
        recv_sem=pair_sem.at[1],
        device_id=(row, col + 1 - 2 * core),
        device_id_type=MESH,
    )
    turn = OWN * (1 - core)
    inverse(1, turn)
    swap.start()

    def second_half(k, carry):
        inverse(1, turn + (2 * core - 1) * k)
        return carry

    lax.fori_loop(1, PLANES, second_half, 0)
    swap.wait()
    load_coupling.wait()

    def finish(p, total):
        value = field[p + 1]
        lap = 6.0 * value - field[p] - field[p + 2]
        for axis in range(2):
            lap = lap - pltpu.roll(value, 1, axis) - pltpu.roll(value, SIZE - 1, axis)
        residual = rhs[p] - (coupling[p] * value + lap)
        solution_ref[p] = value
        residual_ref[p] = residual
        return total + jnp.sum(residual * residual, axis=0, keepdims=True)

    total = lax.fori_loop(0, OWN, finish, jnp.zeros((1, SIZE), F32))
    sums[me] = total[:, :128] + total[:, 128:256] + total[:, 256:384] + total[:, 384:]
    for_partners(me, lambda r, c, t: send(sums.at[me], sums.at[me], 4, r, c))
    for stage in range(4):
        sent(stage)
    most = sums.at[pl.ds(0, DEVICES - 1)]
    pltpu.make_async_copy(most, most, send_sem.at[4]).wait()
    pltpu.make_async_copy(most, most, recv_sem.at[4]).wait()
    norm_ref[...] = jnp.sqrt(jnp.sum(jnp.sum(sums[...], axis=0), axis=1, keepdims=True))


def shards(right_side, coupling):
    held = (OWN, SIZE, SIZE)
    dma = pltpu.SemaphoreType.DMA
    hbm = pl.BlockSpec(memory_space=pltpu.MemorySpace.HBM)
    vmem = pl.BlockSpec(memory_space=pltpu.VMEM)
    solution, residual, norm = pl.pallas_call(
        kernel,
        out_shape=(
            jax.ShapeDtypeStruct(held, F32),
            jax.ShapeDtypeStruct(held, F32),
            jax.ShapeDtypeStruct((1, 1), F32),
        ),
        in_specs=[hbm] * 3,
        out_specs=[vmem] * 3,
        scratch_shapes=[
            pltpu.VMEM(held, F32),
            pltpu.VMEM(held, F32),
            pltpu.VMEM((6, HALF, HALF), BF16),
            pltpu.VMEM((2, 8 * SIZE, 128), F32),
            pltpu.VMEM((2, 8 * SIZE, 128), F32),
            pltpu.VMEM((2, 8 * (SIZE + 2), 128), F32),
            pltpu.VMEM((2, 8 * PLANES * DEVICES, 128), F32),
            pltpu.VMEM((PLANES, SIZE, HALF), F32),
            pltpu.VMEM((OWN + 2, SIZE, SIZE), F32),
            pltpu.VMEM((DEVICES, 1, 128), F32),
            dma((2,)),
            dma((OWN,)),
            dma((4,)),
            dma((5,)),
            dma((5,)),
            dma((2,)),
        ],
        compiler_params=pltpu.CompilerParams(
            collective_id=0, has_side_effects=True, vmem_limit_bytes=44 * 2**20
        ),
    )(right_side, coupling, jnp.asarray(tables()))
    return solution, residual, norm.reshape(1)


def solution(mesh):
    placed = P(ROW_COL, None, None)
    return jax.shard_map(
        shards,
        mesh=mesh,
        in_specs=(placed, placed),
        out_specs=(placed, placed, P()),
        check_vma=False,
    )
```

```python
import math

import jax
import jax.numpy as jnp
import numpy as np
from jax import lax
from jax.experimental import pallas as pl
from jax.experimental.pallas import tpu as pltpu
from jax.sharding import PartitionSpec as P

ROW_COL = ("row", "col")
MESH = pl.DeviceIdType.MESH
SIZE = 512
HALF = SIZE // 2
DEVICES = 128
OWN = SIZE // DEVICES
PLANES = OWN + 1
F32, BF16 = jnp.float32, jnp.bfloat16
EVEN, ODD, ODD_T = 0, 3, 6


def tables():
    n = np.arange(HALF)

    def cas(product):
        angle = 2.0 * math.pi * (product % SIZE) / SIZE
        return np.cos(angle) + np.sin(angle)

    parts = []
    even, odd = cas(n[:, None] * (2 * n)), cas(n[:, None] * (2 * n + 1))
    for table in (even, odd, odd.T):
        for _ in range(3):
            parts.append(table.astype(BF16))
            table = table - parts[-1].astype(np.float64)
    return np.stack(parts)


def split(field, terms):
    parts = []
    for term in range(terms):
        parts.append(field.astype(BF16))
        if term < terms - 1:
            field = field - parts[-1].astype(F32)
    return parts


FORWARD = ((0, 0), (0, 1), (1, 0))
INVERSE = ((0, 0), (0, 1), (0, 2), (1, 0), (1, 1), (2, 0))


def times_right(field, tab, index, pairs):
    parts = split(field, 2 if pairs is FORWARD else 3)
    return jnp.dot(
        jnp.concatenate([parts[d] for d, _ in pairs], axis=1),
        jnp.concatenate([tab[index + t] for _, t in pairs], axis=0),
        preferred_element_type=F32,
    )


def times_left(tab, index, field, pairs):
    parts = split(field, 2 if pairs is FORWARD else 3)
    return jnp.dot(
        jnp.concatenate([tab[index + t] for _, t in pairs], axis=1),
        jnp.concatenate([parts[d] for d, _ in pairs], axis=0),
        preferred_element_type=F32,
    )


def wave(index):
    signed = jnp.where(2 * index < SIZE, index, index - SIZE).astype(F32)
    return jnp.square(signed * (2.0 * math.pi / SIZE))


def partner(me, i):
    core = me & 1
    sign = 1 - 2 * core
    y = (me & 2) | (me >> 4 & 1)
    x = ((me >> 2) + sign * i) & 3
    y = (y + sign * (i + (i >> 2))) & 3
    z = ((me >> 5) + sign * (i + (i >> 4))) & 3
    core = core ^ (i >> 6)
    return z * 2 + (y & 1), x * 4 + (y & 2) + core


def far_first(me, i):
    def offset(k):
        return (1 - (k & 1)) * 2 | ((k ^ (k >> 1)) & 1)

    y = (me & 2) | (me >> 4 & 1)
    z = ((me >> 5) + offset(i >> 5)) & 3
    y = (y + offset(i >> 3 & 3)) & 3
    x = ((me >> 2) + offset(i >> 1 & 3)) & 3
    core = (me & 1) ^ 1 ^ (i & 1)
    return z * 2 + (y & 1), x * 4 + (y & 2) + core


def for_partners(me, act, order=partner, first=1):
    def one(i):
        row, col = order(me, i)
        act(row, col, row * 16 + col)

    def three(k, carry):
        for i in range(3):
            one(first + 3 * k + i)
        return carry

    lax.fori_loop(0, 42, three, 0)
    one(first + 126)


def kernel(
    rhs_hbm, coupling_hbm, tab_hbm,
    solution_ref, residual_ref, norm_ref,
    rhs, coupling, tab, send1, recv1, send2, recv2, part, field, sums,
    load_sem, plane_sem, own_sem, send_sem, recv_sem, pair_sem,
):
    row, col = lax.axis_index("row"), lax.axis_index("col")
    me = row * 16 + col
    core = me & 1
    load_tab = pltpu.make_async_copy(tab_hbm, tab, load_sem.at[0])
    load_coupling = pltpu.make_async_copy(coupling_hbm, coupling, load_sem.at[1])

    def load_plane(p):
        return pltpu.make_async_copy(rhs_hbm.at[p], rhs.at[p], plane_sem.at[p])

    load_tab.start()
    for p in range(OWN):
        load_plane(p).start()

    barrier = pltpu.get_barrier_semaphore()

    def greet(r, c, _):
        pl.semaphore_signal(barrier, inc=1, device_id=(r, c), device_id_type=MESH)

    for_partners(me, greet, far_first, 0)

    def send(src, dst, stage, r, c):
        pltpu.make_async_remote_copy(
            src_ref=src,
            dst_ref=dst,
            send_sem=send_sem.at[stage],
            recv_sem=recv_sem.at[stage],
            device_id=(r, c),
            device_id_type=MESH,
        ).start()

    def rows(start, count):
        return pl.ds(pl.multiple_of(start, 8), count)

    row_mode = lax.broadcasted_iota(jnp.int32, (8, HALF), 0)
    lane_mode = lax.broadcasted_iota(jnp.int32, (8, HALF), 1)

    def forward(h):
        def plane(p, carry):
            if h == 0:
                load_plane(p).wait()
            low, high = rhs[p, :, :HALF], rhs[p, :, HALF:]
            if h == 0:
                both = low + high
                mean = jnp.sum(jnp.sum(both, axis=0, keepdims=True), axis=1, keepdims=True)
                mean = mean * (1.0 / SIZE**2)
                lines = times_right(both - 2.0 * mean, tab, EVEN, FORWARD)
            else:
                lines = times_right(low - high, tab, ODD, FORWARD)
            low, high = lines[:HALF], lines[HALF:]
            for side in range(2):
                if side == 0:
                    modes = times_left(tab, EVEN, low + high, FORWARD)
                    if h == 0:
                        constant = (row_mode == 0) & (lane_mode == 0)
                        top = modes[:8] + jnp.where(constant, mean * float(SIZE**2), 0.0)
                        modes = jnp.concatenate([top, modes[8:]], axis=0)
                else:
                    modes = times_left(tab, ODD_T, low - high, FORWARD)
                for g in range(32):
                    for q in range(2):
                        to = ((side * 32 + g) * 2 + q) * 8 * OWN
                        send1[h, rows(to + p * 8, 8)] = modes[
                            g * 8 : g * 8 + 8, q * 128 : q * 128 + 128
                        ]
            return carry

        lax.fori_loop(0, OWN, plane, 0)

    def send_forward(h):
        def piece(t):
            return send1.at[h, rows(t * 8 * OWN, 8 * OWN)]

        to = recv1.at[h, rows(me * 8 * OWN, 8 * OWN)]
        for_partners(me, lambda r, c, t: send(piece(t), to, h, r, c))
        pltpu.make_async_copy(piece(me), to, own_sem.at[h]).start()

    mode_z = lax.broadcasted_iota(jnp.int32, (HALF, 1), 0) * 2
    waves_z = (wave(mode_z), wave(mode_z + 1))
    lane = lax.broadcasted_iota(jnp.int32, (1, 128), 1)

    def along_z(h):
        wave_x = wave(2 * (me % 2 * 128 + lane) + h)

        def pair(i, carry):
            columns, wave_xy = [], []
            for b in range(2):
                columns.append(recv1[h, pl.ds(2 * i + b, SIZE, stride=8), :])
                order = lane * 0 + (me // 2 * 8 + 2 * i + b)
                mode_y = 2 * order - jnp.where(order < HALF, 0, SIZE - 1)
                wave_xy.append(wave(mode_y) + wave_x)
            lines = jnp.concatenate(columns, axis=1)
            wave_xy = jnp.concatenate(wave_xy, axis=1)
            total = jnp.sum(lines, axis=0, keepdims=True)
            lines = lines - total * (1.0 / SIZE)
            low, high = lines[:HALF], lines[HALF:]

            def scaled(spectrum, wave_z):
                eigen = wave_z + wave_xy
                positive = eigen > 0
                divisor = jnp.where(positive, eigen * float(SIZE**3), 1.0)
                inverse = 1.0 / divisor
                inverse = inverse * (2.0 - divisor * inverse)
                return jnp.where(positive, spectrum * inverse, 0.0)

            even = times_left(tab, EVEN, low + high, FORWARD)
            even = scaled(even + jnp.where(mode_z == 0, total, 0.0), waves_z[0])
            odd = scaled(times_left(tab, ODD_T, low - high, FORWARD), waves_z[1])
            even = times_left(tab, EVEN, even, INVERSE)
            odd = times_left(tab, ODD, odd, INVERSE)
            low, high = even + odd, even - odd
            for b in range(2):
                part_of = slice(b * 128, b * 128 + 128)
                at = 2 * i + b
                send2[h, pl.ds(at + 8, HALF, stride=8), :] = low[:, part_of]
                send2[h, pl.ds(at + 8 + 8 * HALF, HALF, stride=8), :] = high[:, part_of]
                send2[h, pl.ds(at, 1), :] = high[HALF - 1 :, part_of]
                send2[h, pl.ds(at + 8 + 8 * SIZE, 1), :] = low[:1, part_of]
            return carry

        lax.fori_loop(0, 4, pair, 0)

    def group(stage, t):
        side = t & 1
        return {2: (0, 5), 3: (1 - side, 2), 4: (3 - side, 2), 5: (4 * side, 1)}[stage]

    def send_back(stage):
        h = 0 if stage == 2 else 1

        def ends(t):
            j, count = group(stage, t)
            src = send2.at[h, rows((t * OWN + (t & 1) + j) * 8, 8 * count)]
            return src, recv2.at[h, rows((me * PLANES + j) * 8, 8 * count)]

        for_partners(me, lambda r, c, t: send(*ends(t), stage, r, c))
        pltpu.make_async_copy(*ends(me), own_sem.at[stage]).start()

    def bytes_of(stage):
        if stage < 2:
            return recv1.at[stage], 8 * OWN
        return recv2.at[min(stage - 2, 1)], 8 * group(stage, 0)[1]

    def arrived(stage):
        like, own = bytes_of(stage)
        one = like.at[pl.ds(0, own)]
        pltpu.make_async_copy(one, one, own_sem.at[stage]).wait()
        most = like.at[pl.ds(0, (DEVICES - 1) * own)]
        pltpu.make_async_copy(most, most, recv_sem.at[stage]).wait()

    def sent(stage):
        like, own = bytes_of(stage)
        most = like.at[pl.ds(0, (DEVICES - 1) * own)]
        pltpu.make_async_copy(most, most, send_sem.at[stage]).wait()

    def inverse(h, j):
        columns = []
        for q in range(2):
            tiles = [
                recv2[h, rows((g * 2 + q) * 8 * PLANES + j * 8, 8)] for g in range(64)
            ]
            columns.append(jnp.concatenate(tiles, axis=0))
        modes = jnp.concatenate(columns, axis=1)
        even = times_left(tab, EVEN, modes[:HALF], INVERSE)
        odd = times_left(tab, ODD, modes[HALF:], INVERSE)
        lines = jnp.concatenate([even + odd, even - odd], axis=0)
        if h == 0:
            part[j] = times_right(lines, tab, EVEN, INVERSE)
        else:
            odd = times_right(lines, tab, ODD_T, INVERSE)
            even = part[j]
            field[j + core, :, :HALF] = even + odd
            field[j + core, :, HALF:] = even - odd

    load_tab.wait()
    forward(0)
    pl.semaphore_wait(barrier, DEVICES - 1)
    send_forward(0)
    load_coupling.start()
    forward(1)
    send_forward(1)
    arrived(0)
    along_z(0)
    sent(1)
    send_back(2)
    arrived(1)
    along_z(1)
    for stage in (3, 4, 5):
        send_back(stage)

    arrived(2)

    def first_half(j, carry):
        inverse(0, j)
        return carry

    lax.fori_loop(0, PLANES, first_half, 0)
    def second_half(j, carry):
        inverse(1, j)
        return carry

    BLOCK = 64
    row_in = lax.broadcasted_iota(jnp.int32, (8, SIZE), 0)

    def finish(p, total):
        def block(k, total):
            start = k * BLOCK
            here = rows(start, BLOCK)
            value = field[p + 1, here]
            before = field[p + 1, pl.ds((start + SIZE - 1) & (SIZE - 1), 1)]
            after = field[p + 1, pl.ds((start + BLOCK) & (SIZE - 1), 1)]
            up = pltpu.roll(value, 1, 0)
            up = jnp.concatenate([jnp.where(row_in == 0, before, up[:8]), up[8:]], axis=0)
            down = pltpu.roll(value, BLOCK - 1, 0)
            down = jnp.concatenate([down[:-8], jnp.where(row_in == 7, after, down[-8:])], axis=0)
            lap = 6.0 * value - field[p, here] - field[p + 2, here] - up - down
            lap = lap - pltpu.roll(value, 1, 1) - pltpu.roll(value, SIZE - 1, 1)
            residual = rhs[p, here] - (coupling[p, here] * value + lap)
            solution_ref[p, here] = value
            residual_ref[p, here] = residual
            return total + jnp.sum((residual * residual).reshape(BLOCK // 8, 8, SIZE), axis=0)

        return lax.fori_loop(0, SIZE // BLOCK, block, total)

    arrived(3)
    lax.fori_loop(1 - core, 3 - core, second_half, 0)
    arrived(4)
    lax.fori_loop(3 - core, 5 - core, second_half, 0)
    swap = pltpu.make_async_remote_copy(
        src_ref=field.at[OWN - (OWN - 1) * core],
        dst_ref=field.at[(OWN + 1) * core],
        send_sem=pair_sem.at[0],
        recv_sem=pair_sem.at[1],
        device_id=(row, col + 1 - 2 * core),
        device_id_type=MESH,
    )
    swap.start()
    load_coupling.wait()
    total = lax.fori_loop(1, OWN - 1, finish, jnp.zeros((8, SIZE), F32))
    swap.wait()
    total = finish((OWN - 1) * (1 - core), total)
    arrived(5)
    inverse(1, OWN * core)
    total = finish((OWN - 1) * core, total)
    total = jnp.sum(total, axis=0, keepdims=True)
    sums[me] = total[:, :128] + total[:, 128:256] + total[:, 256:384] + total[:, 384:]
    for_partners(me, lambda r, c, t: send(sums.at[me], sums.at[me], 6, r, c), far_first, 0)
    for stage in (0, 2, 3, 4, 5):
        sent(stage)
    most = sums.at[pl.ds(0, DEVICES - 1)]
    pltpu.make_async_copy(most, most, send_sem.at[6]).wait()
    pltpu.make_async_copy(most, most, recv_sem.at[6]).wait()
    norm_ref[...] = jnp.sqrt(jnp.sum(jnp.sum(sums[...], axis=0), axis=1, keepdims=True))


def shards(right_side, coupling):
    held = (OWN, SIZE, SIZE)
    dma = pltpu.SemaphoreType.DMA
    hbm = pl.BlockSpec(memory_space=pltpu.MemorySpace.HBM)
    vmem = pl.BlockSpec(memory_space=pltpu.VMEM)
    solution, residual, norm = pl.pallas_call(
        kernel,
        out_shape=(
            jax.ShapeDtypeStruct(held, F32),
            jax.ShapeDtypeStruct(held, F32),
            jax.ShapeDtypeStruct((1, 1), F32),
        ),
        in_specs=[hbm] * 3,
        out_specs=[vmem] * 3,
        scratch_shapes=[
            pltpu.VMEM(held, F32),
            pltpu.VMEM(held, F32),
            pltpu.VMEM((9, HALF, HALF), BF16),
            pltpu.VMEM((2, 8 * SIZE, 128), F32),
            pltpu.VMEM((2, 8 * SIZE, 128), F32),
            pltpu.VMEM((2, 8 * (SIZE + 2), 128), F32),
            pltpu.VMEM((2, 8 * PLANES * DEVICES, 128), F32),
            pltpu.VMEM((PLANES, SIZE, HALF), F32),
            pltpu.VMEM((OWN + 2, SIZE, SIZE), F32),
            pltpu.VMEM((DEVICES, 1, 128), F32),
            dma((2,)),
            dma((OWN,)),
            dma((6,)),
            dma((7,)),
            dma((7,)),
            dma((2,)),
        ],
        compiler_params=pltpu.CompilerParams(
            collective_id=0, has_side_effects=True, vmem_limit_bytes=44 * 2**20
        ),
    )(right_side, coupling, jnp.asarray(tables()))
    return solution, residual, norm.reshape(1)


def solution(mesh):
    placed = P(ROW_COL, None, None)
    return jax.shard_map(
        shards,
        mesh=mesh,
        in_specs=(placed, placed),
        out_specs=(placed, placed, P()),
        check_vma=False,
    )
```

```python
import math

import jax
import jax.numpy as jnp
import numpy as np
from jax import lax
from jax.experimental import pallas as pl
from jax.experimental.pallas import tpu as pltpu
from jax.sharding import PartitionSpec as P

ROW_COL = ("row", "col")
MESH = pl.DeviceIdType.MESH
SIZE = 512
HALF = SIZE // 2
DEVICES = 128
OWN = SIZE // DEVICES
PLANES = OWN + 1
F32, BF16 = jnp.float32, jnp.bfloat16
EVEN, ODD, ODD_T = 0, 3, 6


def tables():
    n = np.arange(HALF)

    def cas(product):
        angle = 2.0 * math.pi * (product % SIZE) / SIZE
        return np.cos(angle) + np.sin(angle)

    parts = []
    even, odd = cas(n[:, None] * (2 * n)), cas(n[:, None] * (2 * n + 1))
    for table in (even, odd, odd.T):
        for _ in range(3):
            parts.append(table.astype(BF16))
            table = table - parts[-1].astype(np.float64)
    return np.stack(parts)


def split(field, terms):
    parts = []
    for term in range(terms):
        parts.append(field.astype(BF16))
        if term < terms - 1:
            field = field - parts[-1].astype(F32)
    return parts


FORWARD = ((0, 0), (0, 1), (1, 0))
INVERSE = ((0, 0), (0, 1), (0, 2), (1, 0), (1, 1), (2, 0))


def times_right(field, tab, index, pairs):
    parts = split(field, 2 if pairs is FORWARD else 3)
    return jnp.dot(
        jnp.concatenate([parts[d] for d, _ in pairs], axis=1),
        jnp.concatenate([tab[index + t] for _, t in pairs], axis=0),
        preferred_element_type=F32,
    )


def times_left(tab, index, field, pairs):
    parts = split(field, 2 if pairs is FORWARD else 3)
    return jnp.dot(
        jnp.concatenate([tab[index + t] for _, t in pairs], axis=1),
        jnp.concatenate([parts[d] for d, _ in pairs], axis=0),
        preferred_element_type=F32,
    )


def wave(index):
    signed = jnp.where(2 * index < SIZE, index, index - SIZE).astype(F32)
    return jnp.square(signed * (2.0 * math.pi / SIZE))


def partner(me, i):
    core = me & 1
    sign = 1 - 2 * core
    i = i * 37 & 127
    y = (me & 2) | (me >> 4 & 1)
    x = ((me >> 2) + sign * (i)) & 3
    y = (y + sign * (i + (i >> 2))) & 3
    z = ((me >> 5) + sign * (i + (i >> 4))) & 3
    core = core ^ (i >> 6)
    return z * 2 + (y & 1), x * 4 + (y & 2) + core


def far_first(me, i):
    def offset(k):
        return (1 - (k & 1)) * 2 | ((k ^ (k >> 1)) & 1)

    y = (me & 2) | (me >> 4 & 1)
    z = ((me >> 5) + offset(i >> 5)) & 3
    y = (y + offset(i >> 3 & 3)) & 3
    x = ((me >> 2) + offset(i >> 1 & 3)) & 3
    core = (me & 1) ^ 1 ^ (i & 1)
    return z * 2 + (y & 1), x * 4 + (y & 2) + core


def for_partners(me, act, order=partner, first=1):
    def one(i):
        row, col = order(me, i)
        act(row, col, row * 16 + col)

    def three(k, carry):
        for i in range(3):
            one(first + 3 * k + i)
        return carry

    lax.fori_loop(0, 42, three, 0)
    one(first + 126)


def kernel(
    rhs_hbm, coupling_hbm, tab_hbm,
    solution_ref, residual_ref, norm_ref,
    rhs, coupling, tab, send1, recv1, send2, recv2, part, field, sums,
    load_sem, plane_sem, own_sem, send_sem, recv_sem, pair_sem,
):
    row, col = lax.axis_index("row"), lax.axis_index("col")
    me = row * 16 + col
    core = me & 1
    load_tab = pltpu.make_async_copy(tab_hbm, tab, load_sem.at[0])
    load_coupling = pltpu.make_async_copy(coupling_hbm, coupling, load_sem.at[1])

    def load_plane(p):
        return pltpu.make_async_copy(rhs_hbm.at[p], rhs.at[p], plane_sem.at[p])

    load_tab.start()
    for p in range(OWN):
        load_plane(p).start()

    barrier = pltpu.get_barrier_semaphore()

    def greet(r, c, _):
        pl.semaphore_signal(barrier, inc=1, device_id=(r, c), device_id_type=MESH)

    for_partners(me, greet, far_first, 0)

    def send(src, dst, stage, r, c):
        pltpu.make_async_remote_copy(
            src_ref=src,
            dst_ref=dst,
            send_sem=send_sem.at[stage],
            recv_sem=recv_sem.at[stage],
            device_id=(r, c),
            device_id_type=MESH,
        ).start()

    def rows(start, count):
        return pl.ds(pl.multiple_of(start, 8), count)

    row_mode = lax.broadcasted_iota(jnp.int32, (8, HALF), 0)
    lane_mode = lax.broadcasted_iota(jnp.int32, (8, HALF), 1)

    def forward(h):
        def plane(p, carry):
            if h == 0:
                load_plane(p).wait()
            low, high = rhs[p, :, :HALF], rhs[p, :, HALF:]
            if h == 0:
                both = low + high
                mean = jnp.sum(jnp.sum(both, axis=0, keepdims=True), axis=1, keepdims=True)
                mean = mean * (1.0 / SIZE**2)
                lines = times_right(both - 2.0 * mean, tab, EVEN, FORWARD)
            else:
                lines = times_right(low - high, tab, ODD, FORWARD)
            low, high = lines[:HALF], lines[HALF:]
            for side in range(2):
                if side == 0:
                    modes = times_left(tab, EVEN, low + high, FORWARD)
                    if h == 0:
                        constant = (row_mode == 0) & (lane_mode == 0)
                        top = modes[:8] + jnp.where(constant, mean * float(SIZE**2), 0.0)
                        modes = jnp.concatenate([top, modes[8:]], axis=0)
                else:
                    modes = times_left(tab, ODD_T, low - high, FORWARD)
                for g in range(32):
                    for q in range(2):
                        to = ((side * 32 + g) * 2 + q) * 8 * OWN
                        send1[h, rows(to + p * 8, 8)] = modes[
                            g * 8 : g * 8 + 8, q * 128 : q * 128 + 128
                        ]
            return carry

        lax.fori_loop(0, OWN, plane, 0)

    def send_forward(h):
        def piece(t):
            return send1.at[h, rows(t * 8 * OWN, 8 * OWN)]

        to = recv1.at[h, rows(me * 8 * OWN, 8 * OWN)]
        for_partners(me, lambda r, c, t: send(piece(t), to, h, r, c))
        pltpu.make_async_copy(piece(me), to, own_sem.at[h]).start()

    mode_z = lax.broadcasted_iota(jnp.int32, (HALF, 1), 0) * 2
    waves_z = (wave(mode_z), wave(mode_z + 1))
    lane = lax.broadcasted_iota(jnp.int32, (1, 128), 1)

    def along_z(h):
        wave_x = wave(2 * (me % 2 * 128 + lane) + h)

        def pair(i, carry):
            columns, wave_xy = [], []
            for b in range(2):
                columns.append(recv1[h, pl.ds(2 * i + b, SIZE, stride=8), :])
                order = lane * 0 + (me // 2 * 8 + 2 * i + b)
                mode_y = 2 * order - jnp.where(order < HALF, 0, SIZE - 1)
                wave_xy.append(wave(mode_y) + wave_x)
            lines = jnp.concatenate(columns, axis=1)
            wave_xy = jnp.concatenate(wave_xy, axis=1)
            total = jnp.sum(lines, axis=0, keepdims=True)
            lines = lines - total * (1.0 / SIZE)
            low, high = lines[:HALF], lines[HALF:]

            def scaled(spectrum, wave_z):
                eigen = wave_z + wave_xy
                positive = eigen > 0
                divisor = jnp.where(positive, eigen * float(SIZE**3), 1.0)
                inverse = 1.0 / divisor
                inverse = inverse * (2.0 - divisor * inverse)
                return jnp.where(positive, spectrum * inverse, 0.0)

            even = times_left(tab, EVEN, low + high, FORWARD)
            even = scaled(even + jnp.where(mode_z == 0, total, 0.0), waves_z[0])
            odd = scaled(times_left(tab, ODD_T, low - high, FORWARD), waves_z[1])
            even = times_left(tab, EVEN, even, INVERSE)
            odd = times_left(tab, ODD, odd, INVERSE)
            low, high = even + odd, even - odd
            for b in range(2):
                part_of = slice(b * 128, b * 128 + 128)
                at = 2 * i + b
                send2[h, pl.ds(at + 8, HALF, stride=8), :] = low[:, part_of]
                send2[h, pl.ds(at + 8 + 8 * HALF, HALF, stride=8), :] = high[:, part_of]
                send2[h, pl.ds(at, 1), :] = high[HALF - 1 :, part_of]
                send2[h, pl.ds(at + 8 + 8 * SIZE, 1), :] = low[:1, part_of]
            return carry

        lax.fori_loop(0, 4, pair, 0)

    def group(stage, t):
        side = t & 1
        return {2: (0, 5), 3: (1 - side, 2), 4: (3 - side, 2), 5: (4 * side, 1)}[stage]

    def send_back(stage):
        h = 0 if stage == 2 else 1

        def ends(t):
            j, count = group(stage, t)
            src = send2.at[h, rows((t * OWN + (t & 1) + j) * 8, 8 * count)]
            return src, recv2.at[h, rows((me * PLANES + j) * 8, 8 * count)]

        for_partners(me, lambda r, c, t: send(*ends(t), stage, r, c))
        pltpu.make_async_copy(*ends(me), own_sem.at[stage]).start()

    def bytes_of(stage):
        if stage < 2:
            return recv1.at[stage], 8 * OWN
        return recv2.at[min(stage - 2, 1)], 8 * group(stage, 0)[1]

    def arrived(stage):
        like, own = bytes_of(stage)
        one = like.at[pl.ds(0, own)]
        pltpu.make_async_copy(one, one, own_sem.at[stage]).wait()
        most = like.at[pl.ds(0, (DEVICES - 1) * own)]
        pltpu.make_async_copy(most, most, recv_sem.at[stage]).wait()

    def sent(stage):
        like, own = bytes_of(stage)
        most = like.at[pl.ds(0, (DEVICES - 1) * own)]
        pltpu.make_async_copy(most, most, send_sem.at[stage]).wait()

    def inverse(h, j):
        columns = []
        for q in range(2):
            tiles = [
                recv2[h, rows((g * 2 + q) * 8 * PLANES + j * 8, 8)] for g in range(64)
            ]
            columns.append(jnp.concatenate(tiles, axis=0))
        modes = jnp.concatenate(columns, axis=1)
        even = times_left(tab, EVEN, modes[:HALF], INVERSE)
        odd = times_left(tab, ODD, modes[HALF:], INVERSE)
        lines = jnp.concatenate([even + odd, even - odd], axis=0)
        if h == 0:
            part[j] = times_right(lines, tab, EVEN, INVERSE)
        else:
            odd = times_right(lines, tab, ODD_T, INVERSE)
            even = part[j]
            field[j + core, :, :HALF] = even + odd
            field[j + core, :, HALF:] = even - odd

    load_tab.wait()
    forward(0)
    pl.semaphore_wait(barrier, DEVICES - 1)
    send_forward(0)
    load_coupling.start()
    forward(1)
    send_forward(1)
    arrived(0)
    along_z(0)
    sent(1)
    send_back(2)
    arrived(1)
    along_z(1)
    for stage in (3, 4, 5):
        send_back(stage)

    arrived(2)

    def first_half(j, carry):
        inverse(0, j)
        return carry

    lax.fori_loop(0, PLANES, first_half, 0)
    def second_half(j, carry):
        inverse(1, j)
        return carry

    BLOCK = 64
    row_in = lax.broadcasted_iota(jnp.int32, (8, SIZE), 0)

    def finish(p, total):
        def block(k, total):
            start = k * BLOCK
            here = rows(start, BLOCK)
            value = field[p + 1, here]
            before = field[p + 1, pl.ds((start + SIZE - 1) & (SIZE - 1), 1)]
            after = field[p + 1, pl.ds((start + BLOCK) & (SIZE - 1), 1)]
            up = pltpu.roll(value, 1, 0)
            up = jnp.concatenate([jnp.where(row_in == 0, before, up[:8]), up[8:]], axis=0)
            down = pltpu.roll(value, BLOCK - 1, 0)
            down = jnp.concatenate([down[:-8], jnp.where(row_in == 7, after, down[-8:])], axis=0)
            lap = 6.0 * value - field[p, here] - field[p + 2, here] - up - down
            lap = lap - pltpu.roll(value, 1, 1) - pltpu.roll(value, SIZE - 1, 1)
            residual = rhs[p, here] - (coupling[p, here] * value + lap)
            solution_ref[p, here] = value
            residual_ref[p, here] = residual
            return total + jnp.sum((residual * residual).reshape(BLOCK // 8, 8, SIZE), axis=0)

        return lax.fori_loop(0, SIZE // BLOCK, block, total)

    arrived(3)
    lax.fori_loop(1 - core, 3 - core, second_half, 0)
    arrived(4)
    lax.fori_loop(3 - core, 5 - core, second_half, 0)
    swap = pltpu.make_async_remote_copy(
        src_ref=field.at[OWN - (OWN - 1) * core],
        dst_ref=field.at[(OWN + 1) * core],
        send_sem=pair_sem.at[0],
        recv_sem=pair_sem.at[1],
        device_id=(row, col + 1 - 2 * core),
        device_id_type=MESH,
    )
    swap.start()
    load_coupling.wait()
    total = lax.fori_loop(1, OWN - 1, finish, jnp.zeros((8, SIZE), F32))
    swap.wait()
    total = finish((OWN - 1) * (1 - core), total)
    arrived(5)
    inverse(1, OWN * core)
    total = finish((OWN - 1) * core, total)
    total = jnp.sum(total, axis=0, keepdims=True)
    sums[me] = total[:, :128] + total[:, 128:256] + total[:, 256:384] + total[:, 384:]
    for_partners(me, lambda r, c, t: send(sums.at[me], sums.at[me], 6, r, c), far_first, 0)
    for stage in (0, 2, 3, 4, 5):
        sent(stage)
    most = sums.at[pl.ds(0, DEVICES - 1)]
    pltpu.make_async_copy(most, most, send_sem.at[6]).wait()
    pltpu.make_async_copy(most, most, recv_sem.at[6]).wait()
    norm_ref[...] = jnp.sqrt(jnp.sum(jnp.sum(sums[...], axis=0), axis=1, keepdims=True))


def shards(right_side, coupling):
    held = (OWN, SIZE, SIZE)
    dma = pltpu.SemaphoreType.DMA
    hbm = pl.BlockSpec(memory_space=pltpu.MemorySpace.HBM)
    vmem = pl.BlockSpec(memory_space=pltpu.VMEM)
    solution, residual, norm = pl.pallas_call(
        kernel,
        out_shape=(
            jax.ShapeDtypeStruct(held, F32),
            jax.ShapeDtypeStruct(held, F32),
            jax.ShapeDtypeStruct((1, 1), F32),
        ),
        in_specs=[hbm] * 3,
        out_specs=[vmem] * 3,
        scratch_shapes=[
            pltpu.VMEM(held, F32),
            pltpu.VMEM(held, F32),
            pltpu.VMEM((9, HALF, HALF), BF16),
            pltpu.VMEM((2, 8 * SIZE, 128), F32),
            pltpu.VMEM((2, 8 * SIZE, 128), F32),
            pltpu.VMEM((2, 8 * (SIZE + 2), 128), F32),
            pltpu.VMEM((2, 8 * PLANES * DEVICES, 128), F32),
            pltpu.VMEM((PLANES, SIZE, HALF), F32),
            pltpu.VMEM((OWN + 2, SIZE, SIZE), F32),
            pltpu.VMEM((DEVICES, 1, 128), F32),
            dma((2,)),
            dma((OWN,)),
            dma((6,)),
            dma((7,)),
            dma((7,)),
            dma((2,)),
        ],
        compiler_params=pltpu.CompilerParams(
            collective_id=0, has_side_effects=True, vmem_limit_bytes=44 * 2**20
        ),
    )(right_side, coupling, jnp.asarray(tables()))
    return solution, residual, norm.reshape(1)


def solution(mesh):
    placed = P(ROW_COL, None, None)
    return jax.shard_map(
        shards,
        mesh=mesh,
        in_specs=(placed, placed),
        out_specs=(placed, placed, P()),
        check_vma=False,
    )
```

```python
import math

import jax
import jax.numpy as jnp
import numpy as np
from jax import lax
from jax.experimental import pallas as pl
from jax.experimental.pallas import tpu as pltpu
from jax.sharding import PartitionSpec as P

ROW_COL = ("row", "col")
MESH = pl.DeviceIdType.MESH
SIZE = 512
HALF = SIZE // 2
DEVICES = 128
OWN = SIZE // DEVICES
PLANES = OWN + 1
F32, BF16 = jnp.float32, jnp.bfloat16
EVEN, ODD, ODD_T = 0, 3, 6


def tables():
    n = np.arange(HALF)

    def cas(product):
        angle = 2.0 * math.pi * (product % SIZE) / SIZE
        return np.cos(angle) + np.sin(angle)

    parts = []
    even, odd = cas(n[:, None] * (2 * n)), cas(n[:, None] * (2 * n + 1))
    for table in (even, odd, odd.T):
        for _ in range(3):
            parts.append(table.astype(BF16))
            table = table - parts[-1].astype(np.float64)
    return np.stack(parts)


def split(field, terms):
    parts = []
    for term in range(terms):
        parts.append(field.astype(BF16))
        if term < terms - 1:
            field = field - parts[-1].astype(F32)
    return parts


FORWARD = ((0, 0), (0, 1), (1, 0))
INVERSE = ((0, 0), (0, 1), (0, 2), (1, 0), (1, 1), (2, 0))


def times_right(field, tab, index, pairs):
    parts = split(field, 2 if pairs is FORWARD else 3)
    return jnp.dot(
        jnp.concatenate([parts[d] for d, _ in pairs], axis=1),
        jnp.concatenate([tab[index + t] for _, t in pairs], axis=0),
        preferred_element_type=F32,
    )


def times_left(tab, index, field, pairs):
    parts = split(field, 2 if pairs is FORWARD else 3)
    return jnp.dot(
        jnp.concatenate([tab[index + t] for _, t in pairs], axis=1),
        jnp.concatenate([parts[d] for d, _ in pairs], axis=0),
        preferred_element_type=F32,
    )


def wave(index):
    signed = jnp.where(2 * index < SIZE, index, index - SIZE).astype(F32)
    return jnp.square(signed * (2.0 * math.pi / SIZE))


def partner(me, i):
    core = me & 1
    sign = 1 - 2 * core
    i = i * 37 & 127
    y = (me & 2) | (me >> 4 & 1)
    x = ((me >> 2) + sign * (i)) & 3
    y = (y + sign * (i + (i >> 2))) & 3
    z = ((me >> 5) + sign * (i + (i >> 4))) & 3
    core = core ^ (i >> 6)
    return z * 2 + (y & 1), x * 4 + (y & 2) + core


def far_first(me, i):
    def offset(k):
        return (1 - (k & 1)) * 2 | ((k ^ (k >> 1)) & 1)

    y = (me & 2) | (me >> 4 & 1)
    z = ((me >> 5) + offset(i >> 5)) & 3
    y = (y + offset(i >> 3 & 3)) & 3
    x = ((me >> 2) + offset(i >> 1 & 3)) & 3
    core = (me & 1) ^ 1 ^ (i & 1)
    return z * 2 + (y & 1), x * 4 + (y & 2) + core


def for_partners(me, act, order=partner, first=1):
    def one(i):
        row, col = order(me, i)
        act(row, col, row * 16 + col)

    def three(k, carry):
        for i in range(3):
            one(first + 3 * k + i)
        return carry

    lax.fori_loop(0, 42, three, 0)
    one(first + 126)


def kernel(
    rhs_hbm, coupling_hbm, tab_hbm,
    solution_ref, residual_ref, norm_ref,
    rhs, coupling, tab, send1, recv1, send2, recv2, part, field, sums,
    load_sem, plane_sem, own_sem, send_sem, recv_sem, pair_sem,
):
    row, col = lax.axis_index("row"), lax.axis_index("col")
    me = row * 16 + col
    core = me & 1
    load_tab = pltpu.make_async_copy(tab_hbm, tab, load_sem.at[0])
    load_coupling = pltpu.make_async_copy(coupling_hbm, coupling, load_sem.at[1])

    def load_plane(p):
        return pltpu.make_async_copy(rhs_hbm.at[p], rhs.at[p], plane_sem.at[p])

    load_tab.start()
    for p in range(OWN):
        load_plane(p).start()

    barrier = pltpu.get_barrier_semaphore()

    def greet(r, c, _):
        pl.semaphore_signal(barrier, inc=1, device_id=(r, c), device_id_type=MESH)

    for_partners(me, greet, far_first, 0)

    def send(src, dst, stage, r, c):
        pltpu.make_async_remote_copy(
            src_ref=src,
            dst_ref=dst,
            send_sem=send_sem.at[stage],
            recv_sem=recv_sem.at[stage],
            device_id=(r, c),
            device_id_type=MESH,
        ).start()

    def rows(start, count):
        return pl.ds(pl.multiple_of(start, 8), count)

    row_mode = lax.broadcasted_iota(jnp.int32, (8, HALF), 0)
    lane_mode = lax.broadcasted_iota(jnp.int32, (8, HALF), 1)

    def forward(h, first, last):
        def plane(p, carry):
            if h == 0:
                load_plane(p).wait()
            low, high = rhs[p, :, :HALF], rhs[p, :, HALF:]
            if h == 0:
                both = low + high
                mean = jnp.sum(jnp.sum(both, axis=0, keepdims=True), axis=1, keepdims=True)
                mean = mean * (1.0 / SIZE**2)
                lines = times_right(both - 2.0 * mean, tab, EVEN, FORWARD)
            else:
                lines = times_right(low - high, tab, ODD, FORWARD)
            low, high = lines[:HALF], lines[HALF:]
            for side in range(2):
                if side == 0:
                    modes = times_left(tab, EVEN, low + high, FORWARD)
                    if h == 0:
                        constant = (row_mode == 0) & (lane_mode == 0)
                        top = modes[:8] + jnp.where(constant, mean * float(SIZE**2), 0.0)
                        modes = jnp.concatenate([top, modes[8:]], axis=0)
                else:
                    modes = times_left(tab, ODD_T, low - high, FORWARD)
                for g in range(32):
                    for q in range(2):
                        to = ((side * 32 + g) * 2 + q) * 8 * OWN
                        send1[h, rows(to + p * 8, 8)] = modes[
                            g * 8 : g * 8 + 8, q * 128 : q * 128 + 128
                        ]
            return carry

        lax.fori_loop(first, last, plane, 0)

    def send_forward(h, first, last):
        def at(device):
            return h, rows((device * OWN + first) * 8, 8 * (last - first))

        to = recv1.at[at(me)]
        for_partners(me, lambda r, c, t: send(send1.at[at(t)], to, h, r, c))
        if last == OWN:
            whole = rows(me * OWN * 8, 8 * OWN)
            pltpu.make_async_copy(send1.at[h, whole], recv1.at[h, whole], own_sem.at[h]).start()

    mode_z = lax.broadcasted_iota(jnp.int32, (HALF, 1), 0) * 2
    waves_z = (wave(mode_z), wave(mode_z + 1))
    lane = lax.broadcasted_iota(jnp.int32, (1, 128), 1)

    def along_z(h):
        wave_x = wave(2 * (me % 2 * 128 + lane) + h)

        def pair(i, carry):
            columns, wave_xy = [], []
            for b in range(2):
                columns.append(recv1[h, pl.ds(2 * i + b, SIZE, stride=8), :])
                order = lane * 0 + (me // 2 * 8 + 2 * i + b)
                mode_y = 2 * order - jnp.where(order < HALF, 0, SIZE - 1)
                wave_xy.append(wave(mode_y) + wave_x)
            lines = jnp.concatenate(columns, axis=1)
            wave_xy = jnp.concatenate(wave_xy, axis=1)
            total = jnp.sum(lines, axis=0, keepdims=True)
            lines = lines - total * (1.0 / SIZE)
            low, high = lines[:HALF], lines[HALF:]

            def scaled(spectrum, wave_z):
                eigen = wave_z + wave_xy
                positive = eigen > 0
                divisor = jnp.where(positive, eigen * float(SIZE**3), 1.0)
                inverse = 1.0 / divisor
                inverse = inverse * (2.0 - divisor * inverse)
                return jnp.where(positive, spectrum * inverse, 0.0)

            even = times_left(tab, EVEN, low + high, FORWARD)
            even = scaled(even + jnp.where(mode_z == 0, total, 0.0), waves_z[0])
            odd = scaled(times_left(tab, ODD_T, low - high, FORWARD), waves_z[1])
            even = times_left(tab, EVEN, even, INVERSE)
            odd = times_left(tab, ODD, odd, INVERSE)
            low, high = even + odd, even - odd
            for b in range(2):
                part_of = slice(b * 128, b * 128 + 128)
                at = 2 * i + b
                send2[h, pl.ds(at + 8, HALF, stride=8), :] = low[:, part_of]
                send2[h, pl.ds(at + 8 + 8 * HALF, HALF, stride=8), :] = high[:, part_of]
                send2[h, pl.ds(at, 1), :] = high[HALF - 1 :, part_of]
                send2[h, pl.ds(at + 8 + 8 * SIZE, 1), :] = low[:1, part_of]
            return carry

        lax.fori_loop(0, 4, pair, 0)

    def group(stage, t):
        side = t & 1
        return {2: (0, 5), 3: (1 - side, 2), 4: (3 - side, 2), 5: (4 * side, 1)}[stage]

    def send_back(stage):
        h = 0 if stage == 2 else 1

        def ends(t):
            j, count = group(stage, t)
            src = send2.at[h, rows((t * OWN + (t & 1) + j) * 8, 8 * count)]
            return src, recv2.at[h, rows((me * PLANES + j) * 8, 8 * count)]

        for_partners(me, lambda r, c, t: send(*ends(t), stage, r, c))
        pltpu.make_async_copy(*ends(me), own_sem.at[stage]).start()

    def bytes_of(stage):
        if stage < 2:
            return recv1.at[stage], 8 * OWN
        return recv2.at[min(stage - 2, 1)], 8 * group(stage, 0)[1]

    def arrived(stage):
        like, own = bytes_of(stage)
        one = like.at[pl.ds(0, own)]
        pltpu.make_async_copy(one, one, own_sem.at[stage]).wait()
        most = like.at[pl.ds(0, (DEVICES - 1) * own)]
        pltpu.make_async_copy(most, most, recv_sem.at[stage]).wait()

    def sent(stage):
        like, own = bytes_of(stage)
        most = like.at[pl.ds(0, (DEVICES - 1) * own)]
        pltpu.make_async_copy(most, most, send_sem.at[stage]).wait()

    def inverse(h, j):
        columns = []
        for q in range(2):
            tiles = [
                recv2[h, rows((g * 2 + q) * 8 * PLANES + j * 8, 8)] for g in range(64)
            ]
            columns.append(jnp.concatenate(tiles, axis=0))
        modes = jnp.concatenate(columns, axis=1)
        even = times_left(tab, EVEN, modes[:HALF], INVERSE)
        odd = times_left(tab, ODD, modes[HALF:], INVERSE)
        lines = jnp.concatenate([even + odd, even - odd], axis=0)
        if h == 0:
            part[j] = times_right(lines, tab, EVEN, INVERSE)
        else:
            odd = times_right(lines, tab, ODD_T, INVERSE)
            even = part[j]
            field[j + core, :, :HALF] = even + odd
            field[j + core, :, HALF:] = even - odd

    load_tab.wait()
    forward(0, 0, 2)
    pl.semaphore_wait(barrier, DEVICES - 1)
    send_forward(0, 0, 2)
    forward(0, 2, OWN)
    send_forward(0, 2, OWN)
    load_coupling.start()
    forward(1, 0, OWN)
    send_forward(1, 0, OWN)
    arrived(0)
    along_z(0)
    sent(1)
    send_back(2)
    arrived(1)
    along_z(1)
    for stage in (3, 4, 5):
        send_back(stage)

    arrived(2)

    def first_half(j, carry):
        inverse(0, j)
        return carry

    lax.fori_loop(0, PLANES, first_half, 0)
    def second_half(j, carry):
        inverse(1, j)
        return carry

    BLOCK = 64
    row_in = lax.broadcasted_iota(jnp.int32, (8, SIZE), 0)

    def finish(p, total):
        def block(k, total):
            start = k * BLOCK
            here = rows(start, BLOCK)
            value = field[p + 1, here]
            before = field[p + 1, pl.ds((start + SIZE - 1) & (SIZE - 1), 1)]
            after = field[p + 1, pl.ds((start + BLOCK) & (SIZE - 1), 1)]
            up = pltpu.roll(value, 1, 0)
            up = jnp.concatenate([jnp.where(row_in == 0, before, up[:8]), up[8:]], axis=0)
            down = pltpu.roll(value, BLOCK - 1, 0)
            down = jnp.concatenate([down[:-8], jnp.where(row_in == 7, after, down[-8:])], axis=0)
            lap = 6.0 * value - field[p, here] - field[p + 2, here] - up - down
            lap = lap - pltpu.roll(value, 1, 1) - pltpu.roll(value, SIZE - 1, 1)
            residual = rhs[p, here] - (coupling[p, here] * value + lap)
            solution_ref[p, here] = value
            residual_ref[p, here] = residual
            return total + jnp.sum((residual * residual).reshape(BLOCK // 8, 8, SIZE), axis=0)

        return lax.fori_loop(0, SIZE // BLOCK, block, total)

    arrived(3)
    lax.fori_loop(1 - core, 3 - core, second_half, 0)
    arrived(4)
    lax.fori_loop(3 - core, 5 - core, second_half, 0)
    swap = pltpu.make_async_remote_copy(
        src_ref=field.at[OWN - (OWN - 1) * core],
        dst_ref=field.at[(OWN + 1) * core],
        send_sem=pair_sem.at[0],
        recv_sem=pair_sem.at[1],
        device_id=(row, col + 1 - 2 * core),
        device_id_type=MESH,
    )
    swap.start()
    load_coupling.wait()
    total = lax.fori_loop(1, OWN - 1, finish, jnp.zeros((8, SIZE), F32))
    swap.wait()
    total = finish((OWN - 1) * (1 - core), total)
    arrived(5)
    inverse(1, OWN * core)
    total = finish((OWN - 1) * core, total)
    total = jnp.sum(total, axis=0, keepdims=True)
    sums[me] = total[:, :128] + total[:, 128:256] + total[:, 256:384] + total[:, 384:]
    for_partners(me, lambda r, c, t: send(sums.at[me], sums.at[me], 6, r, c), far_first, 0)
    for stage in (0, 2, 3, 4, 5):
        sent(stage)
    most = sums.at[pl.ds(0, DEVICES - 1)]
    pltpu.make_async_copy(most, most, send_sem.at[6]).wait()
    pltpu.make_async_copy(most, most, recv_sem.at[6]).wait()
    norm_ref[...] = jnp.sqrt(jnp.sum(jnp.sum(sums[...], axis=0), axis=1, keepdims=True))


def shards(right_side, coupling):
    held = (OWN, SIZE, SIZE)
    dma = pltpu.SemaphoreType.DMA
    hbm = pl.BlockSpec(memory_space=pltpu.MemorySpace.HBM)
    vmem = pl.BlockSpec(memory_space=pltpu.VMEM)
    solution, residual, norm = pl.pallas_call(
        kernel,
        out_shape=(
            jax.ShapeDtypeStruct(held, F32),
            jax.ShapeDtypeStruct(held, F32),
            jax.ShapeDtypeStruct((1, 1), F32),
        ),
        in_specs=[hbm] * 3,
        out_specs=[vmem] * 3,
        scratch_shapes=[
            pltpu.VMEM(held, F32),
            pltpu.VMEM(held, F32),
            pltpu.VMEM((9, HALF, HALF), BF16),
            pltpu.VMEM((2, 8 * SIZE, 128), F32),
            pltpu.VMEM((2, 8 * SIZE, 128), F32),
            pltpu.VMEM((2, 8 * (SIZE + 2), 128), F32),
            pltpu.VMEM((2, 8 * PLANES * DEVICES, 128), F32),
            pltpu.VMEM((PLANES, SIZE, HALF), F32),
            pltpu.VMEM((OWN + 2, SIZE, SIZE), F32),
            pltpu.VMEM((DEVICES, 1, 128), F32),
            dma((2,)),
            dma((OWN,)),
            dma((6,)),
            dma((7,)),
            dma((7,)),
            dma((2,)),
        ],
        compiler_params=pltpu.CompilerParams(
            collective_id=0, has_side_effects=True, vmem_limit_bytes=44 * 2**20
        ),
    )(right_side, coupling, jnp.asarray(tables()))
    return solution, residual, norm.reshape(1)


def solution(mesh):
    placed = P(ROW_COL, None, None)
    return jax.shard_map(
        shards,
        mesh=mesh,
        in_specs=(placed, placed),
        out_specs=(placed, placed, P()),
        check_vma=False,
    )
```
